32 devices in a mesh: fsdp: 8 (over z, x), tp: 4 (over y, core).
Axes of the slice: x: 2, y: 2, z: 4, core: 2. Of those that a mesh axis runs over, the one named last changes fastest.
Arguments:
- weight_query: bfloat16 [12288, 12288], P('fsdp', 'tp'), may hold values from -0.078125 to 0.078125
- low_query: bfloat16 [12288, 64], P('fsdp'), may hold values from -0.0546875 to 0.0546875
- high_query: bfloat16 [64, 12288], P(None, 'tp'), may hold values from -0.75 to 0.75
- weight_key: bfloat16 [12288, 12288], P('fsdp', 'tp'), may hold values from -0.078125 to 0.078125
- low_key: bfloat16 [12288, 64], P('fsdp'), may hold values from -0.0546875 to 0.0546875
- high_key: bfloat16 [64, 12288], P(None, 'tp'), may hold values from -0.75 to 0.75
- weight_value: bfloat16 [12288, 12288], P('fsdp', 'tp'), may hold values from -0.078125 to 0.078125
- low_value: bfloat16 [12288, 64], P('fsdp'), may hold values from -0.0546875 to 0.0546875
- high_value: bfloat16 [64, 12288], P(None, 'tp'), may hold values from -0.75 to 0.75
- norm_train: float32 [12288], P(('fsdp', 'tp')), may hold values from 0.25 to 1.75
- norm_step: float32 [12288], P(('fsdp', 'tp')), may hold values from -0.3 to 0.3
Outputs:
- ready_query: bfloat16 [12288, 12288], P(None, ('tp', 'fsdp'))
- ready_key: bfloat16 [12288, 12288], P(None, ('tp', 'fsdp'))
- ready_value: bfloat16 [12288, 12288], P(None, ('tp', 'fsdp'))
- factor_query: float32 [12288], P(('tp', 'fsdp'))
- factor_key: float32 [12288], P(('tp', 'fsdp'))
- factor_value: float32 [12288], P(('tp', 'fsdp'))
- serve_norm: bfloat16 [12288], replicated
The draws below stay inside these ranges and needn't reach their ends.
All inputs are finite; a program needn't handle non-finite values. Where the reference program divides by a largest or mean magnitude, that divisor is 1e-20 or more.
Results may differ from the reference program's by a relative error of at most 0.001.
Values may be sent and summed in bfloat16 or wider, within the bound.
A program may use at most 192 MiB of HBM per device.

```python
import jax
import jax.numpy as jnp

D_MODEL = 12288
Q_DIM = 12288
KV_DIM = 12288
RANK = 64


def spiked(result, own_key, source, target, blocks, factor):
    owner, partner = [(jnp.arange(result.shape[position]) // (result.shape[position] // blocks)).reshape([-1 if axis == position else 1 for axis in range(result.ndim)]) for position in (source, target)]
    chosen = jax.random.permutation(own_key, blocks)[partner]
    strong = (owner == chosen) | (owner == (partner + blocks // 2) % blocks)
    return jnp.where(strong, factor * result, result)


def levels(key, shape, cuts, low, high):
    factor_of = 1.0
    for axis_at, shards_of in cuts:
        draws = jax.random.uniform(jax.random.fold_in(jax.random.fold_in(key, 6), axis_at), (shards_of,), jnp.float32, low / len(cuts), high / len(cuts))
        factor_of = factor_of * jnp.repeat(jnp.exp(draws), shape[axis_at] // shards_of).reshape((-1,) + (1,) * (len(shape) - 1 - axis_at))
    return factor_of


def bell_draw(stream_key, shape, deviation, limit, cuts=(), kind=jnp.bfloat16):
    drawn = deviation * jax.random.normal(stream_key, shape, jnp.float32)
    if cuts:
        drawn = drawn * levels(stream_key, shape, cuts, -0.22, 0.18)
    return jnp.clip(drawn, -limit, limit).astype(kind)


def heavy_noise(rng, shape, width, most, cuts, heavy, held_as=jnp.bfloat16):
    values = width * jax.random.normal(rng, shape, jnp.float32)
    if cuts:
        values = values * levels(rng, shape, cuts, -0.22, 0.18)
    return jnp.clip(spiked(values, jax.random.fold_in(rng, 3), *heavy), -most, most).astype(held_as)


def setup_inputs(seed: int = 0) -> dict:
    splits = jax.random.split(jax.random.key(seed), 12)
    weight_query = heavy_noise(splits[0], (D_MODEL, Q_DIM), D_MODEL ** -0.5, 0.078125, ((0, 8), (1, 4)), (0, 1, 8, 2.0))
    low_query = bell_draw(splits[1], (D_MODEL, RANK), D_MODEL ** -0.5, 0.0546875, ((0, 8),))
    high_query = bell_draw(splits[2], (RANK, Q_DIM), RANK ** -0.5, 0.75, ((1, 4),))
    weight_key = heavy_noise(splits[3], (D_MODEL, KV_DIM), D_MODEL ** -0.5, 0.078125, ((0, 8), (1, 4)), (0, 1, 8, 2.0))
    low_key = bell_draw(splits[4], (D_MODEL, RANK), D_MODEL ** -0.5, 0.0546875, ((0, 8),))
    high_key = bell_draw(splits[5], (RANK, KV_DIM), RANK ** -0.5, 0.75, ((1, 4),))
    weight_value = heavy_noise(splits[6], (D_MODEL, KV_DIM), D_MODEL ** -0.5, 0.078125, ((0, 8), (1, 4)), (0, 1, 8, 2.0))
    low_value = bell_draw(splits[7], (D_MODEL, RANK), D_MODEL ** -0.5, 0.0546875, ((0, 8),))
    high_value = bell_draw(splits[8], (RANK, KV_DIM), RANK ** -0.5, 0.75, ((1, 4),))
    norm_train = jnp.clip(1.0 + 0.15 * jax.random.normal(splits[9], (D_MODEL,), jnp.float32), 0.25, 1.75)
    norm_step = jnp.clip(jax.random.uniform(splits[10], (D_MODEL,), jnp.float32, -0.3, 0.3) * levels(splits[10], (D_MODEL,), ((0, 32),), -0.4, 0.0), -0.3, 0.3)
    return dict(weight_query=weight_query, low_query=low_query, high_query=high_query, weight_key=weight_key, low_key=low_key, high_key=high_key, weight_value=weight_value, low_value=low_value, high_value=high_value, norm_train=norm_train, norm_step=norm_step)


mix_rate = 2.0


def reference(weight_query, low_query, high_query, weight_key, low_key, high_key, weight_value, low_value, high_value, norm_train, norm_step):
    latest_query = weight_query.astype(jnp.float32) + mix_rate * jnp.dot(low_query, high_query, preferred_element_type=jnp.float32)
    latest_key = weight_key.astype(jnp.float32) + mix_rate * jnp.dot(low_key, high_key, preferred_element_type=jnp.float32)
    latest_value = weight_value.astype(jnp.float32) + mix_rate * jnp.dot(low_value, high_value, preferred_element_type=jnp.float32)
    factor_query = jnp.max(jnp.abs(latest_query), axis=0)
    ready_query = (latest_query / factor_query).astype(jnp.bfloat16)
    factor_key = jnp.max(jnp.abs(latest_key), axis=0)
    ready_key = (latest_key / factor_key).astype(jnp.bfloat16)
    factor_value = jnp.max(jnp.abs(latest_value), axis=0)
    ready_value = (latest_value / factor_value).astype(jnp.bfloat16)
    serve_norm = (norm_train + norm_step).astype(jnp.bfloat16)
    return ready_query, ready_key, ready_value, factor_query, factor_key, factor_value, serve_norm
```

```python
import functools

import jax
import jax.numpy as jnp
from jax import lax
from jax.experimental import pallas as pl
from jax.experimental.pallas import tpu as pltpu
from jax.sharding import PartitionSpec as P

MESH = pl.DeviceIdType.MESH
LANES = 128


def merge_kernel(
    F,
    T,
    lows_t,
    highs,
    weights,
    norms,
    outs,
    factor_out,
    norm_out,
    low_t,
    high,
    low_s,
    norm_in,
    wbuf,
    sbuf,
    mx,
    in_sem,
    norm_sem,
    load_sem,
    send_sem,
    recv_sem,
    mx_send,
    mx_recv,
    n_send,
    n_recv,
):
    rows = weights[0].shape[0]
    C = outs[0].shape[1]
    K = norm_in.shape[1] // LANES
    subs = C // LANES
    S = len(weights) * subs
    H = F // 2
    G = H // 2
    R = 768 if rows % 768 == 0 else rows
    me = lax.axis_index("fsdp")
    tp = lax.axis_index("tp")
    half, place = me // H, me % H
    z, x = place // 2, place % 2
    turn = z + tp % 2
    f32 = jnp.float32

    def cross(j):
        return (1 - half) * H + (j + turn) % G * 2 + (j // G + x + turn) % 2

    def near(j):
        return half * H + (j + 1 + z) % G * 2 + ((j + 1) // G + x) % 2

    def peer(j):
        return (me + 1 + j) % F

    def other(j):
        return (tp + 1 + j) % T

    barrier = pltpu.get_barrier_semaphore()

    @pl.loop(0, F - 1)
    def _(j):
        pl.semaphore_signal(barrier, inc=1, device_id={"fsdp": peer(j)}, device_id_type=MESH)

    @pl.loop(0, T - 1)
    def _(j):
        pl.semaphore_signal(barrier, inc=1, device_id={"tp": other(j)}, device_id_type=MESH)

    def columns(s, t):
        return pl.ds(pl.multiple_of(t * C + (s % subs) * LANES, LANES), LANES)

    def load(s, slot, t):
        return pltpu.make_async_copy(
            weights[s // subs].at[:, columns(s, t)], wbuf.at[slot, t], load_sem.at[slot, t]
        )

    def start_loads(s, slot):
        @pl.loop(0, F)
        def _(t):
            load(s, slot, t).start()

    def inputs(m):
        return (
            pltpu.make_async_copy(lows_t[m], low_t.at[m], in_sem.at[m, 0]),
            pltpu.make_async_copy(highs[m], high.at[m], in_sem.at[m, 1]),
        )

    def norm_inputs():
        return [pltpu.make_async_copy(norms[i], norm_in.at[i], norm_sem.at[i]) for i in range(2)]

    def merged(s, slot, t, r):
        part = pl.ds(pl.multiple_of(r * R, R), R)
        product = jnp.dot(
            low_s[s // subs, part, :],
            high[s // subs, :, columns(s, t)],
            preferred_element_type=f32,
        )
        return wbuf[slot, t, part, :].astype(f32) + product

    def find_maxima(s, slot):
        @pl.loop(0, F)
        def _(t):
            load(s, slot, t).wait()

            def step(r, most):
                size = jnp.abs(merged(s, slot, t, r))
                return jnp.maximum(most, jnp.max(size.reshape(R // 8, 8, LANES), axis=0))

            most = lax.fori_loop(0, rows // R, step, jnp.zeros((8, LANES), f32))
            mx[s, me, pl.ds(t, 1), :] = jnp.max(most, axis=0, keepdims=True)

    def maxima_copy(group, t, source):
        first, count = groups[group]
        return pltpu.make_async_remote_copy(
            src_ref=mx.at[pl.ds(first, count), me],
            dst_ref=mx.at[pl.ds(first, count), source],
            send_sem=mx_send.at[group, t],
            recv_sem=mx_recv.at[group, source],
            device_id={"fsdp": t},
            device_id_type=MESH,
        )

    groups = [(0, 1), (1, 1), (2, 1), (3, S - 3)]

    def send_maxima(group):
        @pl.loop(0, F - 1)
        def _(j):
            maxima_copy(group, peer(j), me).start()

    def wait_maxima(group):
        @pl.loop(0, F - 1)
        def _(j):
            maxima_copy(group, peer(j), peer(j)).wait_recv()

    def factor(s, t):
        most = mx[s, 0, pl.ds(t, 1), :]
        for source in range(1, F):
            most = jnp.maximum(most, mx[s, source, pl.ds(t, 1), :])
        return most

    def data_copy(s, t, source):
        lanes = pl.ds((s % subs) * LANES, LANES)
        return pltpu.make_async_remote_copy(
            src_ref=sbuf.at[s % 2, t],
            dst_ref=outs[s // subs].at[pl.ds(pl.multiple_of(source * rows, rows), rows), lanes],
            send_sem=send_sem.at[s % 2, t],
            recv_sem=recv_sem.at[s, source],
            device_id={"fsdp": t},
            device_id_type=MESH,
        )

    def scaled(s, slot, t, put):
        load(s, slot, t).wait()
        inverse = 1.0 / factor(s, t)

        @pl.loop(0, rows // R)
        def _(r):
            put(r, (merged(s, slot, t, r) * inverse).astype(jnp.bfloat16))

    def send_block(s, slot, t):
        if s >= 2:
            data_copy(s - 2, t, me).wait_send()

        def put(r, value):
            sbuf[s % 2, t, pl.ds(pl.multiple_of(r * R, R), R), :] = value

        scaled(s, slot, t, put)
        data_copy(s, t, me).start()

    def send_stage(s, slot):
        @pl.loop(0, H - 1)
        def _(j):
            send_block(s, slot, cross(j))
            send_block(s, slot, near(j))

        send_block(s, slot, cross(H - 1))

        def put(r, value):
            lanes = pl.ds((s % subs) * LANES, LANES)
            outs[s // subs][pl.ds(pl.multiple_of(me * rows + r * R, R), R), lanes] = value

        scaled(s, slot, me, put)
        factor_out[s] = factor(s, me)

    visits = [(1, 0), (1, 1), (2, 0), (1, 2), (2, 1)]
    visits += [(1, s) for s in range(3, S)] + [(2, s) for s in range(2, S)]

    for copy in inputs(0):
        copy.start()
    start_loads(0, 0)
    for m in range(1, len(weights)):
        for copy in inputs(m):
            copy.start()
    for copy in norm_inputs():
        copy.start()

    def norm_copy(t, source):
        mine = norm_out.at[source, pl.ds(tp * K, K)]
        return pltpu.make_async_remote_copy(
            src_ref=norm_out.at[me, pl.ds(tp * K, K)],
            dst_ref=mine,
            send_sem=n_send.at[t],
            recv_sem=n_recv.at[source],
            device_id={"fsdp": t},
            device_id_type=MESH,
        )

    greeted = False
    for v, (kind, s) in enumerate(visits):
        slot = v % 2
        if v + 1 < len(visits):
            start_loads(visits[v + 1][1], 1 - slot)
        if kind == 1:
            if s % subs == 0:
                m = s // subs
                for copy in inputs(m):
                    copy.wait()
                low_s[m] = (low_t[m].astype(f32) * 2.0).T.astype(jnp.bfloat16)
            find_maxima(s, slot)
            if not greeted:
                greeted = True
                pl.semaphore_wait(barrier, F + T - 2)
            if s < 3:
                send_maxima(s)
            elif s == S - 1:
                send_maxima(3)
        else:
            if s < 4:
                wait_maxima(s)
            send_stage(s, slot)
        if v == 3:
            for copy in norm_inputs():
                copy.wait()
            for k in range(K):
                part = pl.ds(k * LANES, LANES)
                norm_out[me, tp * K + k] = norm_in[0:1, part] + norm_in[1:2, part]

            @pl.loop(0, F - 1)
            def _(j):
                norm_copy(peer(j), me).start()

    @pl.loop(0, F - 1)
    def _(j):
        norm_copy(peer(j), peer(j)).wait()

    def share(t, source):
        return pltpu.make_async_remote_copy(
            src_ref=norm_out.at[:, pl.ds(tp * K, K)],
            dst_ref=norm_out.at[:, pl.ds(source * K, K)],
            send_sem=n_send.at[F + t],
            recv_sem=n_recv.at[F + source],
            device_id={"tp": t},
            device_id_type=MESH,
        )

    @pl.loop(0, T - 1)
    def _(j):
        share(other(j), tp).start()

    @pl.loop(0, T - 1)
    def _(j):
        share(other(j), other(j)).wait()

    for group in range(4):

        @pl.loop(0, F - 1)
        def _(j):
            maxima_copy(group, peer(j), me).wait_send()

    for s in range(S):

        @pl.loop(0, F - 1)
        def _(j):
            if s >= S - 2:
                data_copy(s, peer(j), me).wait_send()
            data_copy(s, peer(j), peer(j)).wait_recv()


def entry(F, T, *refs):
    lows_t, highs, weights, norms = refs[0:3], refs[3:6], refs[6:9], refs[9:11]
    merge_kernel(F, T, lows_t, highs, weights, norms, refs[11:14], *refs[14:])


def finish_kernel(*refs):
    ready, (factors, norm), ready_out, factor_out = refs[0:3], refs[3:5], refs[5:8], refs[8:11]
    norm_out, factor_buf, norm_buf, ready_sem, small_sem = refs[11:]
    copies = [
        pltpu.make_async_copy(ready[m], ready_out[m], ready_sem.at[m]) for m in range(3)
    ]
    subs = factors.shape[0] // 3
    for copy in copies:
        copy.start()
    for m in range(3):
        factor_buf[m] = factors[m * subs : (m + 1) * subs, 0, :]
        copies.append(pltpu.make_async_copy(factor_buf.at[m], factor_out[m], small_sem.at[m]))
        copies[-1].start()
    norm_buf[...] = norm[:, 0, :].astype(norm_buf.dtype)
    copies.append(pltpu.make_async_copy(norm_buf, norm_out, small_sem.at[3]))
    copies[-1].start()
    for copy in copies:
        copy.wait()


def fused(F, T, wq, lq, hq, wk, lk, hk, wv, lv, hv, norm_train, norm_step):
    rows, width = wq.shape
    rank = lq.shape[1]
    C = width // F
    subs = C // LANES
    S = 3 * subs
    N = norm_train.shape[0]
    K = N // LANES
    f32, bf16 = jnp.float32, jnp.bfloat16
    hbm = pl.BlockSpec(memory_space=pl.ANY)
    vmem = pl.BlockSpec(memory_space=pltpu.VMEM)
    *ready, factors, norm = pl.pallas_call(
        functools.partial(entry, F, T),
        out_shape=[pltpu.VMEM((F * rows, C), bf16)] * 3
        + [pltpu.VMEM((S, 1, LANES), f32), pltpu.VMEM((F, T * K, 1, LANES), f32)],
        in_specs=[hbm] * 11,
        out_specs=[vmem] * 5,
        scratch_shapes=[
            pltpu.VMEM((3, rank, rows), bf16),
            pltpu.VMEM((3, rank, width), bf16),
            pltpu.VMEM((3, rows, rank), bf16),
            pltpu.VMEM((2, N), f32),
            pltpu.VMEM((2, F, rows, LANES), bf16),
            pltpu.VMEM((2, F, rows, LANES), bf16),
            pltpu.VMEM((S, F, F, LANES), f32),
            pltpu.SemaphoreType.DMA((3, 2)),
            pltpu.SemaphoreType.DMA((2,)),
            pltpu.SemaphoreType.DMA((2, F)),
            pltpu.SemaphoreType.DMA((2, F)),
            pltpu.SemaphoreType.DMA((S, F)),
            pltpu.SemaphoreType.DMA((4, F)),
            pltpu.SemaphoreType.DMA((4, F)),
            pltpu.SemaphoreType.DMA((F + T,)),
            pltpu.SemaphoreType.DMA((F + T,)),
        ],
        compiler_params=pltpu.CompilerParams(
            collective_id=0, has_side_effects=True, vmem_limit_bytes=30000000
        ),
    )(lq.T, lk.T, lv.T, hq, hk, hv, wq, wk, wv, norm_train, norm_step)
    norm = norm.reshape(F * T * K, 1, LANES)
    results = pl.pallas_call(
        finish_kernel,
        out_shape=[jax.ShapeDtypeStruct((F * rows, C), bf16)] * 3
        + [jax.ShapeDtypeStruct((subs, LANES), f32)] * 3
        + [jax.ShapeDtypeStruct((F * T * K, LANES), bf16)],
        in_specs=[vmem] * 5,
        out_specs=[hbm] * 7,
        scratch_shapes=[
            pltpu.VMEM((3, subs, LANES), f32),
            pltpu.VMEM((F * T * K, LANES), bf16),
            pltpu.SemaphoreType.DMA((3,)),
            pltpu.SemaphoreType.DMA((4,)),
        ],
        compiler_params=pltpu.CompilerParams(vmem_limit_bytes=2000000),
    )(*[pltpu.with_memory_space_constraint(a, pltpu.VMEM) for a in (*ready, factors, norm)])
    return (*results[:3], *[a.reshape(C) for a in results[3:6]], results[6].reshape(F * T * N))


mix_rate = 2.0


def local(
    weight_query,
    low_query,
    high_query,
    weight_key,
    low_key,
    high_key,
    weight_value,
    low_value,
    high_value,
    norm_train,
    norm_step,
):
    latest_query = weight_query.astype(jnp.float32) + mix_rate * jnp.dot(
        low_query, high_query, preferred_element_type=jnp.float32
    )
    latest_key = weight_key.astype(jnp.float32) + mix_rate * jnp.dot(
        low_key, high_key, preferred_element_type=jnp.float32
    )
    latest_value = weight_value.astype(jnp.float32) + mix_rate * jnp.dot(
        low_value, high_value, preferred_element_type=jnp.float32
    )
    factor_query, factor_key, factor_value = lax.pmax(
        (
            jnp.max(jnp.abs(latest_query), axis=0),
            jnp.max(jnp.abs(latest_key), axis=0),
            jnp.max(jnp.abs(latest_value), axis=0),
        ),
        "fsdp",
    )
    narrow_query, narrow_key, narrow_value = (
        (latest_query / factor_query).astype(jnp.bfloat16),
        (latest_key / factor_key).astype(jnp.bfloat16),
        (latest_value / factor_value).astype(jnp.bfloat16),
    )
    ready_query, ready_key, ready_value = (
        lax.all_to_all(narrow_query, "fsdp", split_axis=1, concat_axis=0, tiled=True),
        lax.all_to_all(narrow_key, "fsdp", split_axis=1, concat_axis=0, tiled=True),
        lax.all_to_all(narrow_value, "fsdp", split_axis=1, concat_axis=0, tiled=True),
    )
    place = lax.axis_index("fsdp")
    factor_query = lax.dynamic_slice_in_dim(
        factor_query, place * ready_query.shape[1], ready_query.shape[1]
    )
    factor_key = lax.dynamic_slice_in_dim(
        factor_key, place * ready_key.shape[1], ready_key.shape[1]
    )
    factor_value = lax.dynamic_slice_in_dim(
        factor_value, place * ready_value.shape[1], ready_value.shape[1]
    )
    serve_norm = lax.all_gather(
        (norm_train + norm_step).astype(jnp.bfloat16), ("fsdp", "tp"), axis=0, tiled=True
    )
    return (ready_query, ready_key, ready_value, factor_query, factor_key, factor_value, serve_norm)


def solution(mesh):
    F, T = mesh.shape["fsdp"], mesh.shape["tp"]

    def step(*args):
        rows, width = args[0].shape
        aligned = width % (F * LANES) == 0 and args[9].shape[0] % LANES == 0
        if not aligned or width < 2 * F * LANES or rows % 16 or F % 4 or T < 2:
            return local(*args)
        return fused(F, T, *args)

    return jax.shard_map(
        step,
        mesh=mesh,
        in_specs=(
            P("fsdp", "tp"),
            P("fsdp", None),
            P(None, "tp"),
            P("fsdp", "tp"),
            P("fsdp", None),
            P(None, "tp"),
            P("fsdp", "tp"),
            P("fsdp", None),
            P(None, "tp"),
            P(("fsdp", "tp")),
            P(("fsdp", "tp")),
        ),
        out_specs=(
            P(None, ("tp", "fsdp")),
            P(None, ("tp", "fsdp")),
            P(None, ("tp", "fsdp")),
            P(("tp", "fsdp")),
            P(("tp", "fsdp")),
            P(("tp", "fsdp")),
            P(),
        ),
        check_vma=False,
    )
```

```python
import functools

import jax
import jax.numpy as jnp
from jax import lax
from jax.experimental import pallas as pl
from jax.experimental.pallas import tpu as pltpu
from jax.sharding import PartitionSpec as P

MESH = pl.DeviceIdType.MESH
LANES = 128
EARLY = 2
AHEAD = 3


def merge_kernel(
    F,
    T,
    lows_t,
    highs,
    weights,
    norms,
    outs,
    factor_out,
    norm_out,
    low_t,
    high,
    low_s,
    norm_in,
    wbuf,
    sbuf,
    first,
    own,
    got,
    fac,
    in_sem,
    norm_sem,
    load_sem,
    send_sem,
    recv_sem,
    mx_send,
    mx_recv,
    low_in,
    early_send,
    early_recv,
    n_send,
    n_recv,
):
    rows = weights[0].shape[0]
    C = outs[0].shape[1]
    K = norm_in.shape[1] // LANES
    subs = C // LANES
    S = len(weights) * subs
    H = F // 2
    G = H // 2
    R = rows if rows <= 1536 else 768 if rows % 768 == 0 else rows
    me = lax.axis_index("fsdp")
    tp = lax.axis_index("tp")
    half, place = me // H, me % H
    z, x = place // 2, place % 2
    turn = z + tp % 2
    f32 = jnp.float32

    def cross(j):
        return (1 - half) * H + (j + turn) % G * 2 + (j // G + x + turn) % 2

    def source(j):
        above = (z - j - tp % 2) % G
        return (1 - half) * H + above * 2 + (x - j // G - above - tp % 2) % 2

    def near(j):
        return half * H + (j + 1 + z) % G * 2 + ((j + 1) // G + x) % 2

    def peer(j):
        return (me + 1 + j) % F

    def other(j):
        return (tp + 1 + j) % T

    barrier = pltpu.get_barrier_semaphore()

    @pl.loop(0, F - 1)
    def _(j):
        pl.semaphore_signal(barrier, inc=1, device_id={"fsdp": peer(j)}, device_id_type=MESH)

    @pl.loop(0, T - 1)
    def _(j):
        pl.semaphore_signal(barrier, inc=1, device_id={"tp": other(j)}, device_id_type=MESH)

    def columns(s, t):
        return pl.ds(pl.multiple_of(t * C + (s % subs) * LANES, LANES), LANES)

    def load(s, slot, t):
        return pltpu.make_async_copy(
            weights[s // subs].at[:, columns(s, t)], wbuf.at[slot, t], load_sem.at[slot, t]
        )

    def start_loads(s, slot):
        @pl.loop(0, F)
        def _(t):
            load(s, slot, t).start()

    def inputs(m):
        return (
            pltpu.make_async_copy(lows_t[m], low_t.at[m], in_sem.at[m, 0]),
            pltpu.make_async_copy(highs[m], high.at[m], in_sem.at[m, 1]),
        )

    def norm_inputs():
        return [pltpu.make_async_copy(norms[i], norm_in.at[i], norm_sem.at[i]) for i in range(2)]

    def merged(s, slot, t, r):
        part = pl.ds(pl.multiple_of(r * R, R), R)
        product = jnp.dot(
            low_s[s // subs, part, :],
            high[s // subs, :, columns(s, t)],
            preferred_element_type=f32,
        )
        return wbuf[slot, t, part, :].astype(f32) + product

    def find_maxima(s, slot):
        @pl.loop(0, F)
        def _(t):
            load(s, slot, t).wait()

            def step(r, most):
                size = jnp.abs(merged(s, slot, t, r))
                return jnp.maximum(most, jnp.max(size.reshape(R // 8, 8, LANES), axis=0))

            most = lax.fori_loop(0, rows // R, step, jnp.zeros((8, LANES), f32))
            most = jnp.max(most, axis=0, keepdims=True)
            own[t, s : s + 1, :] = most
            if s == 0:
                first[me, pl.ds(t, 1), :] = most

    def maxima_copy(kind, t, source):
        pairs = [
            (first.at[me], first.at[source]),
            (own.at[t], got.at[source]),
            (fac.at[me], fac.at[source]),
        ]
        return pltpu.make_async_remote_copy(
            src_ref=pairs[kind][0],
            dst_ref=pairs[kind][1],
            send_sem=mx_send.at[kind, t],
            recv_sem=mx_recv.at[kind, source],
            device_id={"fsdp": t},
            device_id_type=MESH,
        )

    def send_maxima(kind):
        @pl.loop(0, F - 1)
        def _(j):
            maxima_copy(kind, peer(j), me).start()

    def wait_maxima(kind):
        @pl.loop(0, F - 1)
        def _(j):
            maxima_copy(kind, peer(j), peer(j)).wait_recv()

    def reduce_maxima():
        most = own[me]
        for j in range(F - 1):
            most = jnp.maximum(most, got[peer(j)])
        fac[me] = most
        for s in range(S):
            factor_out[s] = most[s : s + 1, :]

    def factor(s, t):
        if s > 0:
            return fac[t, s : s + 1, :]
        most = first[0, pl.ds(t, 1), :]
        for source in range(1, F):
            most = jnp.maximum(most, first[source, pl.ds(t, 1), :])
        return most

    def data_copy(s, t, source, early=False):
        lanes = pl.ds((s % subs) * LANES, LANES)
        skip = LANES if early else 0
        start = pl.multiple_of(source * rows + skip, LANES)
        return pltpu.make_async_remote_copy(
            src_ref=sbuf.at[s % 2, t, pl.ds(skip, rows - skip)],
            dst_ref=outs[s // subs].at[pl.ds(start, rows - skip), lanes],
            send_sem=send_sem.at[s % 2, t],
            recv_sem=recv_sem.at[s, source],
            device_id={"fsdp": t},
            device_id_type=MESH,
        )

    def on_data(s, t, source, j, act):
        if s >= subs or j is None:
            act(data_copy(s, t, source))
        else:

            @pl.when(j < EARLY)
            def _():
                act(data_copy(s, t, source, True))

            @pl.when(j >= EARLY)
            def _():
                act(data_copy(s, t, source))

    def early_copies(j, t, source):
        piece = pl.ds(0, LANES)
        part = pl.ds(pl.multiple_of(source * rows, LANES), LANES)
        wide = pl.ds(pl.multiple_of(t * C, LANES), C)
        pairs = [(weights[0].at[piece, wide], outs[0].at[part]), (lows_t[0].at[:, piece], low_in.at[j])]
        return [
            pltpu.make_async_remote_copy(
                src_ref=src,
                dst_ref=dst,
                send_sem=early_send.at[j, i],
                recv_sem=early_recv.at[j, i],
                device_id={"fsdp": t},
                device_id_type=MESH,
            )
            for i, (src, dst) in enumerate(pairs)
        ]

    def finish_early():
        @pl.loop(0, EARLY)
        def _(j):
            for copy in early_copies(j, cross(j), me):
                copy.wait_send()
            for copy in early_copies(j, source(j), source(j)):
                copy.wait_recv()
            low = (low_in[j].astype(f32) * 2.0).T.astype(jnp.bfloat16)
            part = pl.ds(pl.multiple_of(source(j) * rows, LANES), LANES)
            for s in range(subs):
                lanes = pl.ds(s * LANES, LANES)
                product = jnp.dot(low, high[0, :, columns(s, me)], preferred_element_type=f32)
                value = outs[0][part, lanes].astype(f32) + product
                outs[0][part, lanes] = (value * (1.0 / factor(s, me))).astype(jnp.bfloat16)

    def scaled(s, slot, t, put):
        if s > 0:
            load(s, slot, t).wait()
        inverse = 1.0 / factor(s, t)

        @pl.loop(0, rows // R)
        def _(r):
            put(r, (merged(s, slot, t, r) * inverse).astype(jnp.bfloat16))

    def send_block(s, slot, t, j=None):
        if s >= 2:
            on_data(s - 2, t, me, j, lambda copy: copy.wait_send())

        def put(r, value):
            sbuf[s % 2, t, pl.ds(pl.multiple_of(r * R, R), R), :] = value

        scaled(s, slot, t, put)
        on_data(s, t, me, j, lambda copy: copy.start())

    def send_pairs(s, slot, begin, end):
        @pl.loop(begin, end)
        def _(j):
            send_block(s, slot, cross(j), j)
            send_block(s, slot, near(j))

    def send_last(s, slot):
        send_block(s, slot, cross(H - 1), H - 1)

        def put(r, value):
            lanes = pl.ds((s % subs) * LANES, LANES)
            outs[s // subs][pl.ds(pl.multiple_of(me * rows + r * R, R), R), lanes] = value

        scaled(s, slot, me, put)

    queue = [(kind, s) for kind in (1, 2) for s in range(1, S)]

    def prefetch(v):
        if v < len(queue):
            start_loads(queue[v][1], v % 2)

    def visit_maxima(s, slot):
        if s % subs == 0:
            m = s // subs
            for copy in inputs(m):
                copy.wait()
            low_s[m] = (low_t[m].astype(f32) * 2.0).T.astype(jnp.bfloat16)
        find_maxima(s, slot)

    for copy in inputs(0):
        copy.start()
    start_loads(0, 2)
    prefetch(0)
    for m in range(1, len(weights)):
        for copy in inputs(m):
            copy.start()
    for copy in norm_inputs():
        copy.start()

    def norm_copy(t, source):
        mine = norm_out.at[source, pl.ds(tp * K, K)]
        return pltpu.make_async_remote_copy(
            src_ref=norm_out.at[me, pl.ds(tp * K, K)],
            dst_ref=mine,
            send_sem=n_send.at[t],
            recv_sem=n_recv.at[source],
            device_id={"fsdp": t},
            device_id_type=MESH,
        )

    def send_early(begin, end):
        @pl.loop(begin, end)
        def _(j):
            for copy in early_copies(j, cross(j), me):
                copy.start()

    pl.semaphore_wait(barrier, F + T - 2)
    send_early(0, 1)
    visit_maxima(0, 2)
    send_maxima(0)
    send_early(1, EARLY)
    for s in range(1, S):
        if s == min(AHEAD, S - 1):
            wait_maxima(0)
            send_pairs(0, 2, 0, 1)
        prefetch(s)
        visit_maxima(s, (s - 1) % 2)
    send_maxima(1)
    send_pairs(0, 2, 1, H // 2)
    wait_maxima(1)
    reduce_maxima()
    send_maxima(2)
    send_pairs(0, 2, H // 2, H - 1)
    send_last(0, 2)

    for copy in norm_inputs():
        copy.wait()
    for k in range(K):
        part = pl.ds(k * LANES, LANES)
        norm_out[me, tp * K + k] = norm_in[0:1, part] + norm_in[1:2, part]

    @pl.loop(0, F - 1)
    def _(j):
        norm_copy(peer(j), me).start()

    wait_maxima(2)
    for s in range(1, S):
        v = S - 2 + s
        prefetch(v + 1)
        send_pairs(s, v % 2, 0, H - 1)
        send_last(s, v % 2)
        if s == subs - 1:
            finish_early()

    @pl.loop(0, F - 1)
    def _(j):
        norm_copy(peer(j), peer(j)).wait()

    def share(t, source):
        return pltpu.make_async_remote_copy(
            src_ref=norm_out.at[:, pl.ds(tp * K, K)],
            dst_ref=norm_out.at[:, pl.ds(source * K, K)],
            send_sem=n_send.at[F + t],
            recv_sem=n_recv.at[F + source],
            device_id={"tp": t},
            device_id_type=MESH,
        )

    @pl.loop(0, T - 1)
    def _(j):
        share(other(j), tp).start()

    @pl.loop(0, T - 1)
    def _(j):
        share(other(j), other(j)).wait()

    for kind in range(3):

        @pl.loop(0, F - 1)
        def _(j):
            maxima_copy(kind, peer(j), me).wait_send()

    for s in range(S):

        @pl.loop(0, H)
        def _(j):
            if s >= S - 2:
                data_copy(s, cross(j), me).wait_send()
            on_data(s, source(j), source(j), j, lambda copy: copy.wait_recv())

        @pl.loop(0, H - 1)
        def _(j):
            if s >= S - 2:
                data_copy(s, near(j), me).wait_send()
            data_copy(s, near(j), near(j)).wait_recv()


def entry(F, T, *refs):
    lows_t, highs, weights, norms = refs[0:3], refs[3:6], refs[6:9], refs[9:11]
    merge_kernel(F, T, lows_t, highs, weights, norms, refs[11:14], *refs[14:])


def finish_kernel(*refs):
    ready, (factors, norm), ready_out, factor_out = refs[0:3], refs[3:5], refs[5:8], refs[8:11]
    norm_out, factor_buf, norm_buf, ready_sem, small_sem = refs[11:]
    copies = [
        pltpu.make_async_copy(ready[m], ready_out[m], ready_sem.at[m]) for m in range(3)
    ]
    subs = factors.shape[0] // 3
    for copy in copies:
        copy.start()
    for m in range(3):
        factor_buf[m] = factors[m * subs : (m + 1) * subs, 0, :]
        copies.append(pltpu.make_async_copy(factor_buf.at[m], factor_out[m], small_sem.at[m]))
        copies[-1].start()
    norm_buf[...] = norm[:, 0, :].astype(norm_buf.dtype)
    copies.append(pltpu.make_async_copy(norm_buf, norm_out, small_sem.at[3]))
    copies[-1].start()
    for copy in copies:
        copy.wait()


def fused(F, T, wq, lq, hq, wk, lk, hk, wv, lv, hv, norm_train, norm_step):
    rows, width = wq.shape
    rank = lq.shape[1]
    C = width // F
    subs = C // LANES
    S = 3 * subs
    N = norm_train.shape[0]
    K = N // LANES
    f32, bf16 = jnp.float32, jnp.bfloat16
    hbm = pl.BlockSpec(memory_space=pl.ANY)
    vmem = pl.BlockSpec(memory_space=pltpu.VMEM)
    operands = (lq.T, lk.T, lv.T, hq, hk, hv, wq, wk, wv, norm_train, norm_step)
    *ready, factors, norm = pl.pallas_call(
        functools.partial(entry, F, T),
        out_shape=[pltpu.VMEM((F * rows, C), bf16)] * 3
        + [pltpu.VMEM((S, 1, LANES), f32), pltpu.VMEM((F, T * K, 1, LANES), f32)],
        in_specs=[hbm] * 11,
        out_specs=[vmem] * 5,
        scratch_shapes=[
            pltpu.VMEM((3, rank, rows), bf16),
            pltpu.VMEM((3, rank, width), bf16),
            pltpu.VMEM((3, rows, rank), bf16),
            pltpu.VMEM((2, N), f32),
            pltpu.VMEM((3, F, rows, LANES), bf16),
            pltpu.VMEM((2, F, rows, LANES), bf16),
            pltpu.VMEM((F, F, LANES), f32),
            pltpu.VMEM((F, S, LANES), f32),
            pltpu.VMEM((F, S, LANES), f32),
            pltpu.VMEM((F, S, LANES), f32),
            pltpu.SemaphoreType.DMA((3, 2)),
            pltpu.SemaphoreType.DMA((2,)),
            pltpu.SemaphoreType.DMA((3, F)),
            pltpu.SemaphoreType.DMA((2, F)),
            pltpu.SemaphoreType.DMA((S, F)),
            pltpu.SemaphoreType.DMA((3, F)),
            pltpu.SemaphoreType.DMA((3, F)),
            pltpu.VMEM((EARLY, rank, LANES), bf16),
            pltpu.SemaphoreType.DMA((EARLY, 2)),
            pltpu.SemaphoreType.DMA((EARLY, 2)),
            pltpu.SemaphoreType.DMA((F + T,)),
            pltpu.SemaphoreType.DMA((F + T,)),
        ],
        compiler_params=pltpu.CompilerParams(
            collective_id=0, has_side_effects=True, vmem_limit_bytes=24000000
        ),
    )(*[pltpu.with_memory_space_constraint(a, pltpu.HBM) for a in operands])
    norm = norm.reshape(F * T * K, 1, LANES)
    results = pl.pallas_call(
        finish_kernel,
        out_shape=[jax.ShapeDtypeStruct((F * rows, C), bf16)] * 3
        + [jax.ShapeDtypeStruct((subs, LANES), f32)] * 3
        + [jax.ShapeDtypeStruct((F * T * K, LANES), bf16)],
        in_specs=[vmem] * 5,
        out_specs=[hbm] * 7,
        scratch_shapes=[
            pltpu.VMEM((3, subs, LANES), f32),
            pltpu.VMEM((F * T * K, LANES), bf16),
            pltpu.SemaphoreType.DMA((3,)),
            pltpu.SemaphoreType.DMA((4,)),
        ],
        compiler_params=pltpu.CompilerParams(vmem_limit_bytes=2000000),
    )(*[pltpu.with_memory_space_constraint(a, pltpu.VMEM) for a in (*ready, factors, norm)])
    return (*results[:3], *[a.reshape(C) for a in results[3:6]], results[6].reshape(F * T * N))


mix_rate = 2.0


def local(
    weight_query,
    low_query,
    high_query,
    weight_key,
    low_key,
    high_key,
    weight_value,
    low_value,
    high_value,
    norm_train,
    norm_step,
):
    latest_query = weight_query.astype(jnp.float32) + mix_rate * jnp.dot(
        low_query, high_query, preferred_element_type=jnp.float32
    )
    latest_key = weight_key.astype(jnp.float32) + mix_rate * jnp.dot(
        low_key, high_key, preferred_element_type=jnp.float32
    )
    latest_value = weight_value.astype(jnp.float32) + mix_rate * jnp.dot(
        low_value, high_value, preferred_element_type=jnp.float32
    )
    factor_query, factor_key, factor_value = lax.pmax(
        (
            jnp.max(jnp.abs(latest_query), axis=0),
            jnp.max(jnp.abs(latest_key), axis=0),
            jnp.max(jnp.abs(latest_value), axis=0),
        ),
        "fsdp",
    )
    narrow_query, narrow_key, narrow_value = (
        (latest_query / factor_query).astype(jnp.bfloat16),
        (latest_key / factor_key).astype(jnp.bfloat16),
        (latest_value / factor_value).astype(jnp.bfloat16),
    )
    ready_query, ready_key, ready_value = (
        lax.all_to_all(narrow_query, "fsdp", split_axis=1, concat_axis=0, tiled=True),
        lax.all_to_all(narrow_key, "fsdp", split_axis=1, concat_axis=0, tiled=True),
        lax.all_to_all(narrow_value, "fsdp", split_axis=1, concat_axis=0, tiled=True),
    )
    place = lax.axis_index("fsdp")
    factor_query = lax.dynamic_slice_in_dim(
        factor_query, place * ready_query.shape[1], ready_query.shape[1]
    )
    factor_key = lax.dynamic_slice_in_dim(
        factor_key, place * ready_key.shape[1], ready_key.shape[1]
    )
    factor_value = lax.dynamic_slice_in_dim(
        factor_value, place * ready_value.shape[1], ready_value.shape[1]
    )
    serve_norm = lax.all_gather(
        (norm_train + norm_step).astype(jnp.bfloat16), ("fsdp", "tp"), axis=0, tiled=True
    )
    return (ready_query, ready_key, ready_value, factor_query, factor_key, factor_value, serve_norm)


def solution(mesh):
    F, T = mesh.shape["fsdp"], mesh.shape["tp"]

    def step(*args):
        rows, width = args[0].shape
        aligned = width % (F * LANES) == 0 and args[9].shape[0] % LANES == 0
        if not aligned or width < 2 * F * LANES or rows % LANES or F % 4 or F < 8 or T < 2:
            return local(*args)
        return fused(F, T, *args)

    return jax.shard_map(
        step,
        mesh=mesh,
        in_specs=(
            P("fsdp", "tp"),
            P("fsdp", None),
            P(None, "tp"),
            P("fsdp", "tp"),
            P("fsdp", None),
            P(None, "tp"),
            P("fsdp", "tp"),
            P("fsdp", None),
            P(None, "tp"),
            P(("fsdp", "tp")),
            P(("fsdp", "tp")),
        ),
        out_specs=(
            P(None, ("tp", "fsdp")),
            P(None, ("tp", "fsdp")),
            P(None, ("tp", "fsdp")),
            P(("tp", "fsdp")),
            P(("tp", "fsdp")),
            P(("tp", "fsdp")),
            P(),
        ),
        check_vma=False,
    )
```

```python
import functools

import jax
import jax.numpy as jnp
from jax import lax
from jax.experimental import pallas as pl
from jax.experimental.pallas import tpu as pltpu
from jax.sharding import PartitionSpec as P

MESH = pl.DeviceIdType.MESH
LANES = 128
EARLY = 1
AHEAD = 3
CHUNKS = 2
PARTS = 4


def merge_kernel(
    F,
    T,
    lows_t,
    highs,
    weights,
    norms,
    outs,
    factor_out,
    norm_out,
    low_t,
    high,
    low_s,
    norm_in,
    wbuf,
    sbuf,
    first,
    own,
    got,
    fac,
    in_sem,
    norm_sem,
    load_sem,
    send_sem,
    recv_sem,
    mx_send,
    mx_recv,
    low_in,
    early_send,
    early_recv,
    n_send,
    n_recv,
):
    rows = weights[0].shape[0]
    C = outs[0].shape[1]
    K = norm_in.shape[1] // LANES
    subs = C // LANES
    S = len(weights) * subs
    H = F // 2
    G = H // 2
    R = rows if rows <= 1536 else 768 if rows % 768 == 0 else rows
    rows_c = rows // CHUNKS
    me = lax.axis_index("fsdp")
    tp = lax.axis_index("tp")
    half, place = me // H, me % H
    z, x = place // 2, place % 2
    turn = z + tp % 2
    f32 = jnp.float32

    def cross(j):
        return (1 - half) * H + (j + turn) % G * 2 + (j // G + x + turn) % 2

    def source(j):
        above = (z - j - tp % 2) % G
        return (1 - half) * H + above * 2 + (x - j // G - above - tp % 2) % 2

    def near(j):
        return half * H + (j + 1 + z) % G * 2 + ((j + 1) // G + x) % 2

    def peer(j):
        return (me + 1 + j) % F

    def other(j):
        return (tp + 1 + j) % T

    barrier = pltpu.get_barrier_semaphore()

    @pl.loop(0, F - 1)
    def _(j):
        pl.semaphore_signal(barrier, inc=1, device_id={"fsdp": peer(j)}, device_id_type=MESH)

    @pl.loop(0, T - 1)
    def _(j):
        pl.semaphore_signal(barrier, inc=1, device_id={"tp": other(j)}, device_id_type=MESH)

    def columns(s, t):
        return pl.ds(pl.multiple_of(t * C + (s % subs) * LANES, LANES), LANES)

    def load(s, slot, t):
        return pltpu.make_async_copy(
            weights[s // subs].at[:, columns(s, t)], wbuf.at[slot, t], load_sem.at[slot, t]
        )

    def start_loads(s, slot):
        @pl.loop(0, F)
        def _(t):
            load(s, slot, t).start()

    def inputs(m):
        return (
            pltpu.make_async_copy(lows_t[m], low_t.at[m], in_sem.at[m, 0]),
            pltpu.make_async_copy(highs[m], high.at[m], in_sem.at[m, 1]),
        )

    def norm_inputs():
        return [pltpu.make_async_copy(norms[i], norm_in.at[i], norm_sem.at[i]) for i in range(2)]

    def merged(s, slot, t, part):
        product = jnp.dot(
            low_s[s // subs, part, :],
            high[s // subs, :, columns(s, t)],
            preferred_element_type=f32,
        )
        return wbuf[slot, t, part, :].astype(f32) + product

    def find_maxima(s, slot):
        @pl.loop(0, F)
        def _(t):
            load(s, slot, t).wait()

            def step(r, most):
                size = jnp.abs(merged(s, slot, t, pl.ds(pl.multiple_of(r * R, R), R)))
                return jnp.maximum(most, jnp.max(size.reshape(R // 8, 8, LANES), axis=0))

            most = lax.fori_loop(0, rows // R, step, jnp.zeros((8, LANES), f32))
            most = jnp.max(most, axis=0, keepdims=True)
            own[t, s : s + 1, :] = most
            if s == 0:
                first[me, pl.ds(t, 1), :] = most

    def maxima_copy(kind, t, source):
        pairs = [
            (first.at[me], first.at[source]),
            (own.at[t], got.at[source]),
            (fac.at[me], fac.at[source]),
        ]
        return pltpu.make_async_remote_copy(
            src_ref=pairs[kind][0],
            dst_ref=pairs[kind][1],
            send_sem=mx_send.at[kind, t],
            recv_sem=mx_recv.at[kind, source],
            device_id={"fsdp": t},
            device_id_type=MESH,
        )

    def send_maxima(kind):
        @pl.loop(0, F - 1)
        def _(j):
            maxima_copy(kind, peer(j), me).start()

    def wait_maxima(kind):
        @pl.loop(0, F - 1)
        def _(j):
            maxima_copy(kind, peer(j), peer(j)).wait_recv()

    def reduce_maxima():
        most = own[me]
        for j in range(F - 1):
            most = jnp.maximum(most, got[peer(j)])
        fac[me] = most
        for s in range(S):
            factor_out[s] = most[s : s + 1, :]

    def factor(s, t):
        if s > 0:
            return fac[t, s : s + 1, :]
        most = first[0, pl.ds(t, 1), :]
        for source in range(1, F):
            most = jnp.maximum(most, first[source, pl.ds(t, 1), :])
        return most

    def data_copy(s, t, source, early=False):
        lanes = pl.ds((s % subs) * LANES, LANES)
        skip = LANES if early else 0
        start = pl.multiple_of(source * rows + skip, LANES)
        return pltpu.make_async_remote_copy(
            src_ref=sbuf.at[s % 2, t, pl.ds(skip, rows - skip)],
            dst_ref=outs[s // subs].at[pl.ds(start, rows - skip), lanes],
            send_sem=send_sem.at[s % 2, t, 0],
            recv_sem=recv_sem.at[s, source],
            device_id={"fsdp": t},
            device_id_type=MESH,
        )

    def chunk_copy(s, t, q, early=False):
        lanes = pl.ds((s % subs) * LANES, LANES)
        skip = LANES if early else 0
        begin = pl.multiple_of(q * rows_c + skip, LANES)
        start = pl.multiple_of(me * rows + q * rows_c + skip, LANES)
        return pltpu.make_async_remote_copy(
            src_ref=sbuf.at[s % 2, t, pl.ds(begin, rows_c - skip)],
            dst_ref=outs[s // subs].at[pl.ds(start, rows_c - skip), lanes],
            send_sem=send_sem.at[s % 2, t, q],
            recv_sem=recv_sem.at[s, me],
            device_id={"fsdp": t},
            device_id_type=MESH,
        )

    def on_chunk(s, t, q, j, act):
        if s >= subs or j is None:
            act(chunk_copy(s, t, q))
        else:
            short = (j < EARLY) & (q == 0)

            @pl.when(short)
            def _():
                act(chunk_copy(s, t, q, True))

            @pl.when(jnp.logical_not(short))
            def _():
                act(chunk_copy(s, t, q))

    def wait_data(s, source, j):
        if s >= subs or j is None:
            data_copy(s, source, source).wait_recv()
        else:

            @pl.when(j < EARLY)
            def _():
                data_copy(s, source, source, True).wait_recv()

            @pl.when(j >= EARLY)
            def _():
                data_copy(s, source, source).wait_recv()

    def early_copies(j, t, source):
        piece = pl.ds(0, LANES)
        part = pl.ds(pl.multiple_of(source * rows, LANES), LANES)
        wide = pl.ds(pl.multiple_of(t * C, LANES), C)
        pairs = [(weights[0].at[piece, wide], outs[0].at[part]), (lows_t[0].at[:, piece], low_in.at[j])]
        return [
            pltpu.make_async_remote_copy(
                src_ref=src,
                dst_ref=dst,
                send_sem=early_send.at[j, i],
                recv_sem=early_recv.at[j, i],
                device_id={"fsdp": t},
                device_id_type=MESH,
            )
            for i, (src, dst) in enumerate(pairs)
        ]

    def finish_early():
        @pl.loop(0, EARLY)
        def _(j):
            for copy in early_copies(j, cross(j), me):
                copy.wait_send()
            for copy in early_copies(j, source(j), source(j)):
                copy.wait_recv()
            low = (low_in[j].astype(f32) * 2.0).T.astype(jnp.bfloat16)
            part = pl.ds(pl.multiple_of(source(j) * rows, LANES), LANES)
            for s in range(subs):
                lanes = pl.ds(s * LANES, LANES)
                product = jnp.dot(low, high[0, :, columns(s, me)], preferred_element_type=f32)
                value = outs[0][part, lanes].astype(f32) + product
                outs[0][part, lanes] = (value * (1.0 / factor(s, me))).astype(jnp.bfloat16)

    def send_chunk(s, slot, t, q, j=None):
        if s > 0:

            @pl.when(q == 0)
            def _():
                load(s, slot, t).wait()

        if s >= 2:
            on_chunk(s - 2, t, q, j, lambda copy: copy.wait_send())
        part = pl.ds(pl.multiple_of(q * rows_c, LANES), rows_c)
        value = merged(s, slot, t, part) * (1.0 / factor(s, t))
        sbuf[s % 2, t, part, :] = value.astype(jnp.bfloat16)
        on_chunk(s, t, q, j, lambda copy: copy.start())

    def send_pairs(s, slot, begin, end):
        @pl.loop(0, CHUNKS)
        def _(q):
            @pl.loop(begin, end)
            def _(j):
                send_chunk(s, slot, cross(j), q, j)

                @pl.when(j < H - 1)
                def _():
                    send_chunk(s, slot, near(j % (H - 1)), q)

    def keep_own(s, slot):
        if s > 0:
            load(s, slot, me).wait()
        inverse = 1.0 / factor(s, me)
        lanes = pl.ds((s % subs) * LANES, LANES)

        @pl.loop(0, rows // R)
        def _(r):
            value = merged(s, slot, me, pl.ds(pl.multiple_of(r * R, R), R)) * inverse
            part = pl.ds(pl.multiple_of(me * rows + r * R, R), R)
            outs[s // subs][part, lanes] = value.astype(jnp.bfloat16)

    queue = [(kind, s) for kind in (1, 2) for s in range(1, S)]

    def prefetch(v):
        if v < len(queue):
            start_loads(queue[v][1], v % 2)

    def visit_maxima(s, slot):
        if s % subs == 0:
            m = s // subs
            for copy in inputs(m):
                copy.wait()
            low_s[m] = (low_t[m].astype(f32) * 2.0).T.astype(jnp.bfloat16)
        find_maxima(s, slot)

    for copy in inputs(0):
        copy.start()
    start_loads(0, 2)
    prefetch(0)
    for m in range(1, len(weights)):
        for copy in inputs(m):
            copy.start()
    for copy in norm_inputs():
        copy.start()

    def norm_copy(t, source):
        mine = norm_out.at[source, pl.ds(tp * K, K)]
        return pltpu.make_async_remote_copy(
            src_ref=norm_out.at[me, pl.ds(tp * K, K)],
            dst_ref=mine,
            send_sem=n_send.at[t],
            recv_sem=n_recv.at[source],
            device_id={"fsdp": t},
            device_id_type=MESH,
        )

    def send_early(begin, end):
        @pl.loop(begin, end)
        def _(j):
            for copy in early_copies(j, cross(j), me):
                copy.start()

    visit_maxima(0, 2)
    pl.semaphore_wait(barrier, F + T - 2)
    send_maxima(0)
    send_early(0, EARLY)
    for s in range(1, S):
        if s == min(AHEAD, S - 1):
            wait_maxima(0)
            send_pairs(0, 2, 0, 1)
        prefetch(s)
        visit_maxima(s, (s - 1) % 2)
    send_maxima(1)
    send_pairs(0, 2, 1, H // 2)
    wait_maxima(1)
    reduce_maxima()
    send_maxima(2)
    send_pairs(0, 2, H // 2, H)
    keep_own(0, 2)

    for copy in norm_inputs():
        copy.wait()
    for k in range(K):
        part = pl.ds(k * LANES, LANES)
        norm_out[me, tp * K + k] = norm_in[0:1, part] + norm_in[1:2, part]

    @pl.loop(0, F - 1)
    def _(j):
        norm_copy(peer(j), me).start()

    wait_maxima(2)
    for s in range(1, S):
        v = S - 2 + s
        prefetch(v + 1)
        send_pairs(s, v % 2, 0, H)
        keep_own(s, v % 2)
        if s == subs - 1:
            finish_early()

    @pl.loop(0, F - 1)
    def _(j):
        norm_copy(peer(j), peer(j)).wait()

    def share(t, source):
        return pltpu.make_async_remote_copy(
            src_ref=norm_out.at[:, pl.ds(tp * K, K)],
            dst_ref=norm_out.at[:, pl.ds(source * K, K)],
            send_sem=n_send.at[F + t],
            recv_sem=n_recv.at[F + source],
            device_id={"tp": t},
            device_id_type=MESH,
        )

    @pl.loop(0, T - 1)
    def _(j):
        share(other(j), tp).start()

    @pl.loop(0, T - 1)
    def _(j):
        share(other(j), other(j)).wait()

    for kind in range(3):

        @pl.loop(0, F - 1)
        def _(j):
            maxima_copy(kind, peer(j), me).wait_send()

    for s in range(S):
        if s >= S - 2:

            @pl.loop(0, F - 1)
            def _(j):
                @pl.loop(0, CHUNKS)
                def _(q):
                    chunk_copy(s, peer(j), q).wait_send()

        @pl.loop(0, H)
        def _(j):
            wait_data(s, source(j), j)

        @pl.loop(0, H - 1)
        def _(j):
            wait_data(s, near(j), None)


def entry(F, T, *refs):
    lows_t, highs, weights, norms = refs[0:3], refs[3:6], refs[6:9], refs[9:11]
    merge_kernel(F, T, lows_t, highs, weights, norms, refs[11:14], *refs[14:])


def finish_kernel(*refs):
    ready, (factors, norm), ready_out, factor_out = refs[0:3], refs[3:5], refs[5:8], refs[8:11]
    norm_out, factor_buf, norm_buf, ready_sem, small_sem = refs[11:]
    part = ready[0].shape[0] // PARTS
    copies = [
        pltpu.make_async_copy(
            ready[m].at[pl.ds(p * part, part)],
            ready_out[m].at[pl.ds(p * part, part)],
            ready_sem.at[m, p],
        )
        for p in range(PARTS)
        for m in range(3)
    ]
    subs = factors.shape[0] // 3
    for copy in copies:
        copy.start()
    for m in range(3):
        factor_buf[m] = factors[m * subs : (m + 1) * subs, 0, :]
        copies.append(pltpu.make_async_copy(factor_buf.at[m], factor_out[m], small_sem.at[m]))
        copies[-1].start()
    norm_buf[...] = norm[:, 0, :].astype(norm_buf.dtype)
    copies.append(pltpu.make_async_copy(norm_buf, norm_out, small_sem.at[3]))
    copies[-1].start()
    for copy in copies:
        copy.wait()


def fused(F, T, wq, lq, hq, wk, lk, hk, wv, lv, hv, norm_train, norm_step):
    rows, width = wq.shape
    rank = lq.shape[1]
    C = width // F
    subs = C // LANES
    S = 3 * subs
    N = norm_train.shape[0]
    K = N // LANES
    f32, bf16 = jnp.float32, jnp.bfloat16
    hbm = pl.BlockSpec(memory_space=pl.ANY)
    vmem = pl.BlockSpec(memory_space=pltpu.VMEM)
    operands = (lq.T, lk.T, lv.T, hq, hk, hv, wq, wk, wv, norm_train, norm_step)
    *ready, factors, norm = pl.pallas_call(
        functools.partial(entry, F, T),
        out_shape=[pltpu.VMEM((F * rows, C), bf16)] * 3
        + [pltpu.VMEM((S, 1, LANES), f32), pltpu.VMEM((F, T * K, 1, LANES), f32)],
        in_specs=[hbm] * 11,
        out_specs=[vmem] * 5,
        scratch_shapes=[
            pltpu.VMEM((3, rank, rows), bf16),
            pltpu.VMEM((3, rank, width), bf16),
            pltpu.VMEM((3, rows, rank), bf16),
            pltpu.VMEM((2, N), f32),
            pltpu.VMEM((3, F, rows, LANES), bf16),
            pltpu.VMEM((2, F, rows, LANES), bf16),
            pltpu.VMEM((F, F, LANES), f32),
            pltpu.VMEM((F, S, LANES), f32),
            pltpu.VMEM((F, S, LANES), f32),
            pltpu.VMEM((F, S, LANES), f32),
            pltpu.SemaphoreType.DMA((3, 2)),
            pltpu.SemaphoreType.DMA((2,)),
            pltpu.SemaphoreType.DMA((3, F)),
            pltpu.SemaphoreType.DMA((2, F, CHUNKS)),
            pltpu.SemaphoreType.DMA((S, F)),
            pltpu.SemaphoreType.DMA((3, F)),
            pltpu.SemaphoreType.DMA((3, F)),
            pltpu.VMEM((EARLY, rank, LANES), bf16),
            pltpu.SemaphoreType.DMA((EARLY, 2)),
            pltpu.SemaphoreType.DMA((EARLY, 2)),
            pltpu.SemaphoreType.DMA((F + T,)),
            pltpu.SemaphoreType.DMA((F + T,)),
        ],
        compiler_params=pltpu.CompilerParams(
            collective_id=0, has_side_effects=True, vmem_limit_bytes=24000000
        ),
    )(*[pltpu.with_memory_space_constraint(a, pltpu.HBM) for a in operands])
    norm = norm.reshape(F * T * K, 1, LANES)
    results = pl.pallas_call(
        finish_kernel,
        out_shape=[jax.ShapeDtypeStruct((F * rows, C), bf16)] * 3
        + [jax.ShapeDtypeStruct((subs, LANES), f32)] * 3
        + [jax.ShapeDtypeStruct((F * T * K, LANES), bf16)],
        in_specs=[vmem] * 5,
        out_specs=[hbm] * 7,
        scratch_shapes=[
            pltpu.VMEM((3, subs, LANES), f32),
            pltpu.VMEM((F * T * K, LANES), bf16),
            pltpu.SemaphoreType.DMA((3, PARTS)),
            pltpu.SemaphoreType.DMA((4,)),
        ],
        compiler_params=pltpu.CompilerParams(vmem_limit_bytes=2000000),
    )(*[pltpu.with_memory_space_constraint(a, pltpu.VMEM) for a in (*ready, factors, norm)])
    return (*results[:3], *[a.reshape(C) for a in results[3:6]], results[6].reshape(F * T * N))


mix_rate = 2.0


def local(
    weight_query,
    low_query,
    high_query,
    weight_key,
    low_key,
    high_key,
    weight_value,
    low_value,
    high_value,
    norm_train,
    norm_step,
):
    latest_query = weight_query.astype(jnp.float32) + mix_rate * jnp.dot(
        low_query, high_query, preferred_element_type=jnp.float32
    )
    latest_key = weight_key.astype(jnp.float32) + mix_rate * jnp.dot(
        low_key, high_key, preferred_element_type=jnp.float32
    )
    latest_value = weight_value.astype(jnp.float32) + mix_rate * jnp.dot(
        low_value, high_value, preferred_element_type=jnp.float32
    )
    factor_query, factor_key, factor_value = lax.pmax(
        (
            jnp.max(jnp.abs(latest_query), axis=0),
            jnp.max(jnp.abs(latest_key), axis=0),
            jnp.max(jnp.abs(latest_value), axis=0),
        ),
        "fsdp",
    )
    narrow_query, narrow_key, narrow_value = (
        (latest_query / factor_query).astype(jnp.bfloat16),
        (latest_key / factor_key).astype(jnp.bfloat16),
        (latest_value / factor_value).astype(jnp.bfloat16),
    )
    ready_query, ready_key, ready_value = (
        lax.all_to_all(narrow_query, "fsdp", split_axis=1, concat_axis=0, tiled=True),
        lax.all_to_all(narrow_key, "fsdp", split_axis=1, concat_axis=0, tiled=True),
        lax.all_to_all(narrow_value, "fsdp", split_axis=1, concat_axis=0, tiled=True),
    )
    place = lax.axis_index("fsdp")
    factor_query = lax.dynamic_slice_in_dim(
        factor_query, place * ready_query.shape[1], ready_query.shape[1]
    )
    factor_key = lax.dynamic_slice_in_dim(
        factor_key, place * ready_key.shape[1], ready_key.shape[1]
    )
    factor_value = lax.dynamic_slice_in_dim(
        factor_value, place * ready_value.shape[1], ready_value.shape[1]
    )
    serve_norm = lax.all_gather(
        (norm_train + norm_step).astype(jnp.bfloat16), ("fsdp", "tp"), axis=0, tiled=True
    )
    return (ready_query, ready_key, ready_value, factor_query, factor_key, factor_value, serve_norm)


def solution(mesh):
    F, T = mesh.shape["fsdp"], mesh.shape["tp"]

    def step(*args):
        rows, width = args[0].shape
        aligned = width % (F * LANES) == 0 and args[9].shape[0] % LANES == 0
        if not aligned or width < 2 * F * LANES or rows % (CHUNKS * LANES) or F % 4 or F < 8 or T < 2:
            return local(*args)
        return fused(F, T, *args)

    return jax.shard_map(
        step,
        mesh=mesh,
        in_specs=(
            P("fsdp", "tp"),
            P("fsdp", None),
            P(None, "tp"),
            P("fsdp", "tp"),
            P("fsdp", None),
            P(None, "tp"),
            P("fsdp", "tp"),
            P("fsdp", None),
            P(None, "tp"),
            P(("fsdp", "tp")),
            P(("fsdp", "tp")),
        ),
        out_specs=(
            P(None, ("tp", "fsdp")),
            P(None, ("tp", "fsdp")),
            P(None, ("tp", "fsdp")),
            P(("tp", "fsdp")),
            P(("tp", "fsdp")),
            P(("tp", "fsdp")),
            P(),
        ),
        check_vma=False,
    )
```
